32 devices in a mesh: dp: 8 (over z, y), cp: 4 (over x, core).
Axes of the slice: x: 2, y: 2, z: 4, core: 2. Of those that a mesh axis runs over, the one named last changes fastest.
Arguments:
- x_in: bfloat16 [8, 4096, 1024], P('dp', 'cp')
- d_out: bfloat16 [8, 4096, 1024], P('dp', 'cp')
- w_q: bfloat16 [1024, 16, 64], replicated
- w_k: bfloat16 [1024, 16, 64], replicated
- w_v: bfloat16 [1024, 16, 64], replicated
- w_o: bfloat16 [16, 64, 1024], replicated
- w_up: bfloat16 [1024, 4096], replicated
- w_down: bfloat16 [4096, 1024], replicated
Outputs:
- output 1: bfloat16 [8, 4096, 1024], P('dp', 'cp')
- output 2: float32 [1024, 16, 64], replicated
- output 3: float32 [1024, 16, 64], replicated
- output 4: float32 [1024, 16, 64], replicated
- output 5: float32 [16, 64, 1024], replicated
- output 6: float32 [1024, 4096], replicated
- output 7: float32 [4096, 1024], replicated
All inputs are finite; a program needn't handle non-finite values.
Results may differ from the reference program's by a relative error of at most 0.0176615.
Values are sent between devices in bfloat16 or wider.
A program may use at most 1 GiB of HBM per device.

```python
import jax
import jax.numpy as jnp
from jax import lax

BATCH_SIZE = 8
SEQ_LEN = 4096
D_MODEL = 1024
N_HEADS = 16
HEAD_DIM = 64
FFN_DIM = 4096
N_SHARDS = 32
Q_BLOCK = 512


def setup_inputs(seed: int = 0) -> dict:
    key_list = jax.random.split(jax.random.key(seed), 8)
    attn_width = N_HEADS * HEAD_DIM
    act_shape = (BATCH_SIZE, SEQ_LEN, D_MODEL)

    def draw_normal(key_part, arr_shape, std_dev):
        return (jax.random.normal(key_part, arr_shape, jnp.float32) * std_dev).astype(jnp.bfloat16)

    return {
        'x_in': draw_normal(key_list[0], act_shape, 1.0),
        'd_out': draw_normal(key_list[1], act_shape, 1.0),
        'w_q': draw_normal(key_list[2], (D_MODEL, N_HEADS, HEAD_DIM), D_MODEL ** -0.5),
        'w_k': draw_normal(key_list[3], (D_MODEL, N_HEADS, HEAD_DIM), D_MODEL ** -0.5),
        'w_v': draw_normal(key_list[4], (D_MODEL, N_HEADS, HEAD_DIM), D_MODEL ** -0.5),
        'w_o': draw_normal(key_list[5], (N_HEADS, HEAD_DIM, D_MODEL), attn_width ** -0.5),
        'w_up': draw_normal(key_list[6], (D_MODEL, FFN_DIM), D_MODEL ** -0.5),
        'w_down': draw_normal(key_list[7], (FFN_DIM, D_MODEL), FFN_DIM ** -0.5),
    }


def keep_bf16(values):
    return values.astype(jnp.bfloat16).astype(jnp.float32)


def stored_positions():
    n_blocks = SEQ_LEN // Q_BLOCK
    stored = jnp.arange(n_blocks)
    owner_rank = stored // 2
    seq_block = owner_rank + (stored % 2) * (n_blocks - 1 - 2 * owner_rank)
    return (seq_block[:, None] * Q_BLOCK + jnp.arange(Q_BLOCK)[None, :]).reshape(SEQ_LEN)


def attend_block(q_rows, pos_rows, key_seq, val_seq, positions):
    scores = jnp.einsum('qhe,khe->hqk', q_rows, key_seq) * (HEAD_DIM ** -0.5)
    scores = jnp.where(positions[None, None, :] <= pos_rows[None, :, None], scores, -1e30)
    prob_b = keep_bf16(jax.nn.softmax(scores, axis=-1))
    return keep_bf16(jnp.einsum('hqk,khe->qhe', prob_b, val_seq))


def attend_sequence(q_seq, key_seq, val_seq, positions):
    n_blocks = SEQ_LEN // Q_BLOCK
    q_blocks = q_seq.reshape(n_blocks, Q_BLOCK, N_HEADS, HEAD_DIM)
    pos_blocks = positions.reshape(n_blocks, Q_BLOCK)
    block_fn = jax.checkpoint(attend_block)
    outs = lax.map(lambda block_pair: block_fn(block_pair[0], block_pair[1], key_seq, val_seq, positions), (q_blocks, pos_blocks))
    return outs.reshape(SEQ_LEN, N_HEADS, HEAD_DIM)


def reference(x_in, d_out, w_q, w_k, w_v, w_o, w_up, w_down):
    positions = stored_positions()

    def forward(x_f32, wq_f32, wk_f32, wv_f32, wo_f32, wu_f32, wd_f32):
        q_seq = keep_bf16(jnp.einsum('bsd,dhe->bshe', x_f32, wq_f32))
        k_seq = keep_bf16(jnp.einsum('bsd,dhe->bshe', x_f32, wk_f32))
        v_seq = keep_bf16(jnp.einsum('bsd,dhe->bshe', x_f32, wv_f32))
        attn_out = lax.map(lambda qkv_rows: attend_sequence(qkv_rows[0], qkv_rows[1], qkv_rows[2], positions), (q_seq, k_seq, v_seq))
        hidden = keep_bf16(x_f32 + jnp.einsum('bshe,hed->bsd', attn_out, wo_f32))
        up_pre = keep_bf16(jnp.einsum('bsd,df->bsf', hidden, wu_f32))
        act_val = keep_bf16(jax.nn.gelu(up_pre, approximate=True))
        return (hidden + jnp.einsum('bsf,fd->bsd', act_val, wd_f32)).astype(jnp.bfloat16)

    out_val, pullback = jax.vjp(
        forward,
        x_in.astype(jnp.float32),
        w_q.astype(jnp.float32),
        w_k.astype(jnp.float32),
        w_v.astype(jnp.float32),
        w_o.astype(jnp.float32),
        w_up.astype(jnp.float32),
        w_down.astype(jnp.float32),
    )
    grads = pullback(d_out)
    return (
        grads[0].astype(jnp.bfloat16),
        grads[1] / N_SHARDS,
        grads[2] / N_SHARDS,
        grads[3] / N_SHARDS,
        grads[4] / N_SHARDS,
        grads[5] / N_SHARDS,
        grads[6] / N_SHARDS,
    )
```

```python
import functools
import jax
import jax.numpy as jnp
from jax import lax
from jax.experimental import pallas as pl
from jax.experimental.pallas import tpu as pltpu
from jax.sharding import PartitionSpec as P


LOG2E = 1.4426950408889634
NEG_BIG = -1e30
BLK = 512
F32 = jnp.float32
BF16 = jnp.bfloat16


def nt(a, b):
    return lax.dot_general(a, b, (((1,), (1,)), ((), ())), preferred_element_type=F32)


def nn(a, b):
    return lax.dot_general(a, b, (((1,), (0,)), ((), ())), preferred_element_type=F32)


def lane_mask(half):
    lanes = lax.broadcasted_iota(jnp.int32, (BLK, 128), 1)
    return (lanes < 64) if half == 0 else (lanes >= 64)


def pick(arr, half):
    return jnp.where(lane_mask(half), arr, jnp.zeros_like(arr))


def load_all(srcs, dsts, sem):
    copies = []
    for parts, dst in zip(srcs, dsts):
        for j, (ref, c) in enumerate(parts):
            rows = ref.shape[0]
            copies.append(pltpu.make_async_copy(ref.at[:, pl.ds(c, 128)], dst.at[pl.ds(j * rows, rows), :], sem))
    for c in copies:
        c.start()
    for c in copies:
        c.wait()


def attn_fwd_kernel(pair, tab_ref, *refs):
    qkv_refs = refs[:4]
    o_ref, lse_ref, q_ref, k_ref, v_ref, vt_ref, sem = refs[4:]
    n_blk = q_ref.shape[0] // BLK
    step = pl.program_id(0)

    @pl.when(step == 0)
    def _():
        load_all([[(r, 384 * pair + 128 * t) for r in qkv_refs] for t in range(3)], [q_ref, k_ref, v_ref], sem)
        for b in range(n_blk):
            rows = pl.ds(b * BLK, BLK)
            vt_ref[:, rows] = v_ref[rows, :].astype(F32).T.astype(BF16)

    q_off = pl.multiple_of(tab_ref[step] * BLK, BLK)
    q_blk = q_ref[pl.ds(q_off, BLK), :] * jnp.asarray(0.125, BF16)
    q_half = [pick(q_blk, 0), pick(q_blk, 1)]

    def update(key_idx, state, diag):
        off = pl.multiple_of(tab_ref[key_idx] * BLK, BLK)
        k_blk = k_ref[pl.ds(off, BLK), :]
        out = []
        for h in range(2):
            m_row, l_row, acc = state[3 * h:3 * h + 3]
            s = nt(k_blk, q_half[h])
            if diag:
                kk = lax.broadcasted_iota(jnp.int32, (BLK, BLK), 0)
                qq = lax.broadcasted_iota(jnp.int32, (BLK, BLK), 1)
                s = jnp.where(kk <= qq, s, NEG_BIG)
            m_new = jnp.maximum(m_row, jnp.max(s, axis=0, keepdims=True))
            fac = jnp.exp2((m_row - m_new) * LOG2E)
            p = jnp.exp2((s - m_new) * LOG2E)
            l_row = l_row * fac + jnp.sum(p, axis=0, keepdims=True)
            vt = vt_ref[64 * h:64 * h + 64, pl.ds(off, BLK)]
            acc = acc * fac + nn(vt, p.astype(BF16))
            out += [m_new, l_row, acc]
        return tuple(out)

    fresh = (jnp.full((1, BLK), NEG_BIG, F32), jnp.zeros((1, BLK), F32), jnp.zeros((64, BLK), F32))
    state = lax.fori_loop(0, step, lambda j, st: update(j, st, False), fresh + fresh)
    state = update(step, state, True)
    o_t = jnp.concatenate([state[2] / state[1], state[5] / state[4]], axis=0)
    o_ref[pl.ds(q_off, BLK), :] = o_t.T.astype(BF16)
    for h in range(2):
        lse_ref[0, h:h + 1, pl.ds(q_off, BLK)] = (state[3 * h] + jnp.log(state[3 * h + 1])) * LOG2E


def attn_bwd_kernel(pair, tab_ref, *refs):
    qkv_refs, do_refs = refs[:4], refs[4:8]
    o_ref, lse_ref = refs[8:10]
    out_refs = refs[10:14]
    q_ref, k_ref, v_ref, do_ref, dqt_ref, dot_ref, dkv_ref, sem = refs[14:]
    n_blk = q_ref.shape[0] // BLK
    step = pl.program_id(0)

    @pl.when(step == 0)
    def _():
        load_all([[(r, 384 * pair + 128 * t) for r in qkv_refs] for t in range(3)] + [[(r, 0) for r in do_refs]],
                 [q_ref, k_ref, v_ref, do_ref], sem)
        dqt_ref[...] = jnp.zeros_like(dqt_ref)
        for b in range(n_blk):
            rows = pl.ds(b * BLK, BLK)
            prod = (do_ref[rows, :].astype(F32) * o_ref[rows, :].astype(F32)).T
            dot_ref[0:1, rows] = jnp.sum(prod[:64], axis=0, keepdims=True)
            dot_ref[1:2, rows] = jnp.sum(prod[64:], axis=0, keepdims=True)

    k_off = pl.multiple_of(tab_ref[step] * BLK, BLK)
    k_blk = k_ref[pl.ds(k_off, BLK), :]
    v_blk = v_ref[pl.ds(k_off, BLK), :]
    k_t = k_blk.astype(F32).T.astype(BF16)

    def update(q_idx, state, diag):
        dk, dv = state
        off = pl.multiple_of(tab_ref[q_idx] * BLK, BLK)
        q_blk = q_ref[pl.ds(off, BLK), :] * jnp.asarray(0.125, BF16)
        do_blk = do_ref[pl.ds(off, BLK), :]
        for h in range(2):
            q_h = pick(q_blk, h)
            do_h = pick(do_blk, h)
            s = nt(k_blk, q_h)
            if diag:
                kk = lax.broadcasted_iota(jnp.int32, (BLK, BLK), 0)
                qq = lax.broadcasted_iota(jnp.int32, (BLK, BLK), 1)
                s = jnp.where(kk <= qq, s, NEG_BIG)
            p = jnp.exp2(s * LOG2E - lse_ref[0, h:h + 1, pl.ds(off, BLK)])
            dp = nt(v_blk, do_h).astype(BF16).astype(F32)
            ds = (p * (dp - dot_ref[h:h + 1, pl.ds(off, BLK)])).astype(BF16)
            dv = dv + nn(p.astype(BF16), do_h)
            dk = dk + nn(ds, q_h)
            cols = pl.ds(off, BLK)
            dqt_ref[64 * h:64 * h + 64, cols] += nn(k_t[64 * h:64 * h + 64], ds)
        return dk, dv

    zero = jnp.zeros((BLK, 128), F32)
    state = update(step, (zero, zero), True)
    dk, dv = lax.fori_loop(step + 1, n_blk, lambda i, st: update(i, st, False), state)
    dkv_ref[pl.ds(k_off, BLK), 0:128] = dk.astype(BF16)
    dkv_ref[pl.ds(k_off, BLK), 128:256] = dv.astype(BF16)

    @pl.when(step == n_blk - 1)
    def _():
        rows = q_ref.shape[0] // 4
        for j in range(4):
            span = pl.ds(j * rows, rows)
            out_refs[j][:, 0:128] = (dqt_ref[:, span] * 0.125).T.astype(BF16)
            out_refs[j][:, 128:384] = dkv_ref[span, :]


def pair_cost(seq_len, n_dots):
    return pl.CostEstimate(flops=2 * seq_len * seq_len * 128 * n_dots * 2, bytes_accessed=16 * seq_len * 128,
                           transcendentals=seq_len * seq_len)


ANY = pl.BlockSpec(memory_space=pl.ANY)


def attn_fwd(tab, qkv, pair):
    rows = qkv[0].shape[0]
    seq_len = 4 * rows
    n_blk = seq_len // BLK
    whole = pl.BlockSpec((seq_len, 128), lambda i, tab: (0, 0))
    buf = pltpu.VMEM((seq_len, 128), BF16)
    return pl.pallas_call(
        functools.partial(attn_fwd_kernel, pair),
        out_shape=[jax.ShapeDtypeStruct((seq_len, 128), BF16), jax.ShapeDtypeStruct((1, 2, seq_len), F32)],
        grid_spec=pltpu.PrefetchScalarGridSpec(
            num_scalar_prefetch=1, grid=(n_blk,),
            in_specs=[ANY] * 4,
            out_specs=[whole, pl.BlockSpec((1, 2, seq_len), lambda i, tab: (0, 0, 0))],
            scratch_shapes=[buf, buf, buf, pltpu.VMEM((128, seq_len), BF16), pltpu.SemaphoreType.DMA]),
        compiler_params=pltpu.CompilerParams(vmem_limit_bytes=48 * 1024 * 1024),
        cost_estimate=pair_cost(seq_len, 2),
        name='attn_fwd')(tab, *qkv)


def attn_bwd(tab, qkv, d_o, out_o, lse, pair):
    rows = qkv[0].shape[0]
    seq_len = 4 * rows
    n_blk = seq_len // BLK
    whole = pl.BlockSpec((seq_len, 128), lambda i, tab: (0, 0))
    buf = pltpu.VMEM((seq_len, 128), BF16)
    return pl.pallas_call(
        functools.partial(attn_bwd_kernel, pair),
        out_shape=[jax.ShapeDtypeStruct((rows, 384), BF16)] * 4,
        grid_spec=pltpu.PrefetchScalarGridSpec(
            num_scalar_prefetch=1, grid=(n_blk,),
            in_specs=[ANY] * 8 + [whole, pl.BlockSpec((1, 2, seq_len), lambda i, tab: (0, 0, 0))],
            out_specs=[pl.BlockSpec((rows, 384), lambda i, tab: (0, 0))] * 4,
            scratch_shapes=[buf, buf, buf, buf, pltpu.VMEM((128, seq_len), F32), pltpu.VMEM((2, seq_len), F32),
                            pltpu.VMEM((seq_len, 256), BF16), pltpu.SemaphoreType.DMA]),
        compiler_params=pltpu.CompilerParams(vmem_limit_bytes=48 * 1024 * 1024),
        cost_estimate=pair_cost(seq_len, 5),
        name='attn_bwd')(tab, *qkv, *d_o, out_o, lse)


MESH = pl.DeviceIdType.MESH
LAG = 2
UNIT = 256
WIDE = 1024


def sum_kernel(up_ref, mine_ref, up_out, qkv_out, acc, rc, r1, r2, rz, macc, my, mz,
               one, pairs, tri_s, tri_r, tri_as, tri_ar, m_one, m_pairs, m_tri_s, m_tri_r, m_tri_as, m_tri_ar):
    dp, cp = lax.axis_index('dp'), lax.axis_index('cp')
    z, y, x, c = dp // 2, dp % 2, cp // 2, cp % 2
    n_up, n_mine = acc.shape[0], macc.shape[0]
    blocks = up_ref.shape[1] // WIDE
    ids = lambda d, p: {'dp': d, 'cp': p}
    core_id = ids(dp, 2 * x + 1 - c)
    x_id = ids(dp, 2 * (1 - x) + c)
    y_id = ids(2 * z + 1 - y, cp)
    z_ids = [ids(2 * ((z + k) % 4) + y, cp) for k in (1, 2, 3)]

    barrier = pltpu.get_barrier_semaphore()
    for peer in [core_id, x_id, y_id] + z_ids:
        pl.semaphore_signal(barrier, inc=1, device_id=peer, device_id_type=MESH)
    pl.semaphore_wait(barrier, 6)

    def remote(src, dst, s_sem, r_sem, dev):
        return pltpu.make_async_remote_copy(src_ref=src, dst_ref=dst, send_sem=s_sem, recv_sem=r_sem,
                                            device_id=dev, device_id_type=MESH)

    class Up:
        def __init__(self, u):
            color = u % 2
            self.u = u
            self.row = (u // blocks) * UNIT
            self.cols = pl.ds(pl.multiple_of((u % blocks) * WIDE, WIDE), WIDE)
            self.b1 = x + color * (y - x)
            self.b2 = y + color * (x - y)
            self.d1 = ids(2 * z + y + color * (1 - 2 * y), 2 * (x + (1 - color) * (1 - 2 * x)) + c)
            self.d2 = ids(2 * z + y + (1 - color) * (1 - 2 * y), 2 * (x + color * (1 - 2 * x)) + c)
            self.base = self.b1 * (UNIT // 4) + self.b2 * (UNIT // 8)

        def src(self, off, n):
            return up_ref.at[pl.ds(pl.multiple_of(self.row + off, 8), n), self.cols]

        def out(self, off, n):
            return up_out.at[pl.ds(pl.multiple_of(self.row + off, 8), n), self.cols]

        def part(self, off, n):
            return acc.at[self.u, pl.ds(pl.multiple_of(off, 8), n), :]

        def pair(self, i, src, dst, dev):
            return remote(src, dst, pairs.at[self.u, i, 0], pairs.at[self.u, i, 1], dev)

        def load(self):
            return pltpu.make_async_copy(self.src(c * (UNIT // 2), UNIT // 2), acc.at[self.u], one.at[self.u, 0])

        def core(self):
            return self.pair(0, self.src((1 - c) * (UNIT // 2), UNIT // 2), rc.at[self.u], core_id)

        def first(self):
            return self.pair(1, self.part((1 - self.b1) * (UNIT // 4), UNIT // 4), r1.at[self.u], self.d1)

        def second(self):
            return self.pair(2, self.part(self.b1 * (UNIT // 4) + (1 - self.b2) * (UNIT // 8), UNIT // 8),
                             r2.at[self.u], self.d2)

        def zs(self):
            n = UNIT // 32
            return [remote(self.part(self.base + ((z + k) % 4) * n, n), rz.at[self.u, k - 1],
                           tri_s.at[self.u, k - 1], tri_r.at[self.u, k - 1], z_ids[k - 1]) for k in (1, 2, 3)]

        def back_zs(self):
            n = UNIT // 32
            dst = self.out(c * (UNIT // 2) + self.base + z * n, n)
            return [remote(self.part(self.base + z * n, n), dst,
                           tri_as.at[self.u, k - 1], tri_ar.at[self.u, k - 1], z_ids[k - 1]) for k in (1, 2, 3)]

        def keep(self):
            n = UNIT // 32
            return pltpu.make_async_copy(self.part(self.base + z * n, n),
                                         self.out(c * (UNIT // 2) + self.base + z * n, n), one.at[self.u, 1])

        def back(self, i, off, n, dev):
            return self.pair(i, self.out(off, n), self.out(off, n), dev)

        def back_second(self):
            return self.back(3, c * (UNIT // 2) + self.base, UNIT // 8, self.d2)

        def back_first(self):
            return self.back(4, c * (UNIT // 2) + self.b1 * (UNIT // 4), UNIT // 4, self.d1)

        def back_core(self):
            return self.back(5, c * (UNIT // 2), UNIT // 2, core_id)

    def add_into(ref, other):
        ref[...] = ref[...] + other[...]

    def up_take(s, u):
        w = Up(u)
        if s == 1:
            w.load().wait()
            w.core().wait_recv()
            add_into(acc.at[u], rc.at[u])
        elif s == 2:
            w.first().wait_recv()
            add_into(w.part(w.b1 * (UNIT // 4), UNIT // 4), r1.at[u])
        elif s == 3:
            w.second().wait_recv()
            add_into(w.part(w.base, UNIT // 8), r2.at[u])
        elif s == 4:
            for cpy in w.zs():
                cpy.wait_recv()
            n = UNIT // 32
            dst = w.part(w.base + z * n, n)
            dst[...] = dst[...] + (rz[u, 0] + rz[u, 1] + rz[u, 2])
        elif s == 5:
            for cpy in w.back_zs():
                cpy.wait_recv()
            w.keep().wait()
        elif s == 6:
            w.back_second().wait_recv()
        elif s == 7:
            w.back_first().wait_recv()
        elif s == 8:
            w.back_core().wait_recv()
            for cpy in [w.core(), w.first(), w.second()] + w.zs() + w.back_zs() + [
                    w.back_second(), w.back_first(), w.back_core()]:
                cpy.wait_send()

    def up_give(s, u):
        w = Up(u)
        todo = [lambda: [w.load(), w.core()], lambda: [w.first()], lambda: [w.second()], w.zs,
                lambda: w.back_zs() + [w.keep()], lambda: [w.back_second()], lambda: [w.back_first()],
                lambda: [w.back_core()]][s]
        for cpy in todo():
            cpy.start()

    class Mine:
        def __init__(self, m):
            self.m = m
            self.orow = (m // 4) * 1024 + (m % 4) * 64

        def out(self, holder, off, n):
            return qkv_out.at[pl.ds(pl.multiple_of(self.orow + holder * 256 + off, 8), n), :]

        def part(self, off, n):
            return macc.at[self.m, pl.ds(pl.multiple_of(off, 8), n), :]

        def pair(self, i, src, dst, dev):
            return remote(src, dst, m_pairs.at[self.m, i, 0], m_pairs.at[self.m, i, 1], dev)

        def load(self):
            return pltpu.make_async_copy(mine_ref.at[pl.ds(pl.multiple_of(self.m * 64, 8), 64), :], macc.at[self.m],
                                         m_one.at[self.m, 0])

        def ys(self):
            return self.pair(0, mine_ref.at[pl.ds(pl.multiple_of(self.m * 64 + (1 - y) * 32, 8), 32), :],
                             my.at[self.m], y_id)

        def zs(self):
            return [remote(self.part(y * 32 + ((z + k) % 4) * 8, 8), mz.at[self.m, k - 1],
                           m_tri_s.at[self.m, k - 1], m_tri_r.at[self.m, k - 1], z_ids[k - 1]) for k in (1, 2, 3)]

        def back_zs(self):
            return [remote(self.part(y * 32 + z * 8, 8), self.out(cp, y * 32 + z * 8, 8),
                           m_tri_as.at[self.m, k - 1], m_tri_ar.at[self.m, k - 1], z_ids[k - 1]) for k in (1, 2, 3)]

        def keep(self):
            return pltpu.make_async_copy(self.part(y * 32 + z * 8, 8), self.out(cp, y * 32 + z * 8, 8),
                                         m_one.at[self.m, 1])

        def back_y(self):
            return self.pair(1, self.out(cp, y * 32, 32), self.out(cp, y * 32, 32), y_id)

        def back_x(self):
            return self.pair(2, self.out(cp, 0, 64), self.out(cp, 0, 64), x_id)

        def back_core(self):
            return self.pair(3, self.out(cp, 0, 64), self.out(cp, 0, 64), core_id)

        def back_far(self):
            far = 2 * (1 - x) + c
            return self.pair(4, self.out(far, 0, 64), self.out(far, 0, 64), core_id)

    def mine_take(s, m):
        w = Mine(m)
        if s == 1:
            w.load().wait()
            w.ys().wait_recv()
            add_into(w.part(y * 32, 32), my.at[m])
        elif s == 2:
            for cpy in w.zs():
                cpy.wait_recv()
            dst = w.part(y * 32 + z * 8, 8)
            dst[...] = dst[...] + (mz[m, 0] + mz[m, 1] + mz[m, 2])
        elif s == 3:
            for cpy in w.back_zs():
                cpy.wait_recv()
            w.keep().wait()
        elif s == 4:
            w.back_y().wait_recv()
        elif s == 5:
            w.back_x().wait_recv()
        elif s == 6:
            w.back_core().wait_recv()
            w.back_far().wait_recv()
            for cpy in [w.ys()] + w.zs() + w.back_zs() + [w.back_y(), w.back_x(), w.back_core(), w.back_far()]:
                cpy.wait_send()

    def mine_give(s, m):
        w = Mine(m)
        todo = [lambda: [w.load(), w.ys()], w.zs, lambda: w.back_zs() + [w.keep()], lambda: [w.back_y()],
                lambda: [w.back_x(), w.back_core()], lambda: [w.back_far()]][s]
        for cpy in todo():
            cpy.start()

    def at_step(fn, t, s, n):
        u = t - LAG * s

        @pl.when((u >= 0) & (u < n))
        def _():
            fn(s, u)

    def step(t, carry):
        for s in range(8, 0, -1):
            at_step(up_take, t, s, n_up)
        for s in range(6, 0, -1):
            at_step(mine_take, t, s, n_mine)
        for s in range(7, -1, -1):
            at_step(up_give, t, s, n_up)
        for s in range(5, -1, -1):
            at_step(mine_give, t, s, n_mine)
        return carry

    lax.fori_loop(0, max(n_up + 8 * LAG, n_mine + 6 * LAG), step, 0)


def sum_grads(up, mine):
    n_up = up.shape[0] * up.shape[1] // (UNIT * WIDE)
    n_mine = mine.shape[0] // 64
    cols = mine.shape[1]
    dma = pltpu.SemaphoreType.DMA
    vm = lambda *shape: pltpu.VMEM(shape, F32)
    return pl.pallas_call(
        sum_kernel,
        out_shape=[jax.ShapeDtypeStruct(up.shape, F32), jax.ShapeDtypeStruct((4 * mine.shape[0], cols), F32)],
        in_specs=[ANY] * 2, out_specs=[ANY] * 2,
        scratch_shapes=[vm(n_up, UNIT // 2, WIDE), vm(n_up, UNIT // 2, WIDE), vm(n_up, UNIT // 4, WIDE),
                        vm(n_up, UNIT // 8, WIDE), vm(n_up, 3, UNIT // 32, WIDE),
                        vm(n_mine, 64, cols), vm(n_mine, 32, cols), vm(n_mine, 3, 8, cols),
                        dma((n_up, 2)), dma((n_up, 6, 2))] + [dma((n_up, 3))] * 4
                       + [dma((n_mine, 2)), dma((n_mine, 5, 2))] + [dma((n_mine, 3))] * 4,
        compiler_params=pltpu.CompilerParams(collective_id=0, has_side_effects=True,
                                             vmem_limit_bytes=56 * 1024 * 1024),
        cost_estimate=pl.CostEstimate(flops=200 * 10 ** 9, bytes_accessed=2 ** 26, transcendentals=0),
        name='sum_grads')(up, mine)


def tn(a, b):
    return lax.dot_general(a, b, (((0,), (0,)), ((), ())), preferred_element_type=F32)


def solution(mesh):
    cp_size = mesh.shape['cp']
    n_total = mesh.shape['dp'] * cp_size
    inv = 1.0 / n_total

    def flip(arr, bit):
        return lax.ppermute(arr, 'cp', [(i, i ^ bit) for i in range(cp_size)]) if bit else arr

    def per_device(x_in, d_out, w_q, w_k, w_v, w_o, w_up, w_down):
        rank = lax.axis_index('cp')
        x_own, g_out = x_in[0], d_out[0]
        tokens, d_model = x_own.shape
        width = d_model // cp_size
        n_pairs = width // 128
        w_t = [jnp.transpose(w, (1, 2, 0)).reshape(d_model // 128, 1, 128, d_model) for w in (w_q, w_k, w_v)]
        w_qkv = jnp.concatenate(w_t, axis=1).reshape(3 * d_model, d_model)
        wo2 = w_o.reshape(d_model, d_model)
        w_mine = lax.dynamic_slice(w_qkv, (rank * 3 * width, 0), (3 * width, d_model))
        slots = range(cp_size)

        x_all = [x_own, flip(x_own, 1), flip(x_own, 2)]
        grad_act = nt(g_out, w_down).astype(BF16)
        x_far, grad_act = lax.optimization_barrier((x_all[2], grad_act))
        x_all = [x_all[0], x_all[1], x_far, flip(x_far, 1)]
        seq_blk = jnp.arange(2 * cp_size)
        holder = jnp.where(seq_blk < cp_size, seq_blk, 2 * cp_size - 1 - seq_blk)
        tab = (2 * jnp.bitwise_xor(holder, rank) + (seq_blk >= cp_size)).astype(jnp.int32)
        qkv = [nt(x_j, w_mine).astype(BF16) for x_j in x_all]

        def absolute(parts, w):
            rel = jnp.concatenate(parts, axis=1)
            return jnp.concatenate([lax.dynamic_slice(rel, (0, (b ^ rank) * w), (tokens, w)) for b in slots], axis=1)

        attn_o, lses, o_parts = [], [], {}
        for pair in range(n_pairs):
            o_pair, lse = attn_fwd(tab, qkv, pair)
            attn_o.append(o_pair)
            lses.append(lse)
            for j in slots:
                o_parts[j, pair] = flip(o_pair[j * tokens:(j + 1) * tokens], j)
        o_own = absolute([o_parts[j, p] for j in slots for p in range(n_pairs)], width)

        hidden = (x_own.astype(F32) + nn(o_own, wo2)).astype(BF16)
        up_pre = nn(hidden, w_up).astype(BF16)
        act_val, gelu_pull = jax.vjp(functools.partial(jax.nn.gelu, approximate=True), up_pre.astype(F32))
        act_b = act_val.astype(BF16)
        grad_pre = gelu_pull(grad_act.astype(F32))[0].astype(BF16)
        grad_down = tn(act_b, g_out) * inv
        grad_hidden = (g_out.astype(F32) + nt(grad_pre, w_up)).astype(BF16)
        grad_attn = nt(grad_hidden, wo2).astype(BF16)
        grad_up = tn(hidden, grad_pre) * inv
        grad_o = tn(o_own, grad_hidden) * inv

        d_o = []
        for pair in range(n_pairs):
            pieces = [lax.dynamic_slice(grad_attn, (0, (rank ^ j) * width + 128 * pair), (tokens, 128)) for j in slots]
            d_o.append([flip(pieces[j], j) for j in slots])
        d_o[0], grad_down, grad_up, grad_o = lax.optimization_barrier((d_o[0], grad_down, grad_up, grad_o))
        grad_down, grad_o = lax.psum((grad_down, grad_o), ('dp', 'cp'))

        grads, back = [], {}
        for pair in range(n_pairs):
            parts = attn_bwd(tab, qkv, d_o[pair], attn_o[pair], lses[pair], pair)
            for j in slots:
                back[j, pair] = flip(parts[j], j)
            grads.append(sum(tn(parts[j], x_all[j]) for j in slots) * inv)
        mine = jnp.concatenate(grads, axis=0).reshape(n_pairs, 3, 128, d_model)
        mine = jnp.transpose(mine, (1, 0, 2, 3)).reshape(3 * width, d_model)
        grad_up, g_qkv = sum_grads(grad_up, mine)
        outs = [jnp.transpose(g_qkv[t * d_model:(t + 1) * d_model].reshape(w.shape[1], w.shape[2], d_model), (2, 0, 1))
                for t, w in enumerate((w_q, w_k, w_v))]
        back_abs = absolute([back[j, p] for j in slots for p in range(n_pairs)], 3 * width)
        d_x = (grad_hidden.astype(F32) + nn(back_abs, w_qkv)).astype(BF16)
        return (d_x[None], *outs, grad_o.reshape(w_o.shape), grad_up, grad_down)

    act_spec = P('dp', 'cp', None)
    return jax.shard_map(per_device, mesh=mesh,
                         in_specs=(act_spec, act_spec, P(), P(), P(), P(), P(), P()),
                         out_specs=(act_spec, P(), P(), P(), P(), P(), P()),
                         check_vma=False)
```

```python
import functools
import jax
import jax.numpy as jnp
from jax import lax
from jax.experimental import pallas as pl
from jax.experimental.pallas import tpu as pltpu
from jax.sharding import PartitionSpec as P


LOG2E = 1.4426950408889634
NEG_BIG = -1e30
BLK = 512
F32 = jnp.float32
BF16 = jnp.bfloat16


def nt(a, b):
    return lax.dot_general(a, b, (((1,), (1,)), ((), ())), preferred_element_type=F32)


def nn(a, b):
    return lax.dot_general(a, b, (((1,), (0,)), ((), ())), preferred_element_type=F32)


def lane_mask(half):
    lanes = lax.broadcasted_iota(jnp.int32, (BLK, 128), 1)
    return (lanes < 64) if half == 0 else (lanes >= 64)


def pick(arr, half):
    return jnp.where(lane_mask(half), arr, jnp.zeros_like(arr))


def load_all(srcs, dsts, sem):
    copies = []
    for parts, dst in zip(srcs, dsts):
        for b, (ref, row, col) in enumerate(parts):
            copies.append(pltpu.make_async_copy(ref.at[pl.ds(row, BLK), pl.ds(col, 128)],
                                                dst.at[pl.ds(b * BLK, BLK), :], sem))
    for c in copies:
        c.start()
    for c in copies:
        c.wait()


def attn_fwd_kernel(pair, n_in, first, tab_ref, *refs):
    qkv_refs, o_refs = refs[:n_in], refs[n_in:n_in + 4]
    lse_ref, q_ref, k_ref, v_ref, vt_ref, o_ref, sem = refs[n_in + 4:]
    step = pl.program_id(0)
    seq = step + first

    @pl.when(step == 0)
    def _():
        load_all([[(r, 0, 384 * pair + 128 * t) for r in (qkv_refs if t else qkv_refs[n_in - 4:])] for t in range(3)],
                 [q_ref, k_ref, v_ref], sem)
        for b in range(n_in):
            rows = pl.ds(b * BLK, BLK)
            vt_ref[:, rows] = v_ref[rows, :].astype(F32).T.astype(BF16)

    q_off = pl.multiple_of((tab_ref[seq] - first) * BLK, BLK)
    q_blk = q_ref[pl.ds(q_off, BLK), :] * jnp.asarray(0.125, BF16)
    q_half = [pick(q_blk, 0), pick(q_blk, 1)]

    def update(key_idx, state, diag):
        off = pl.multiple_of(tab_ref[key_idx] * BLK, BLK)
        k_blk = k_ref[pl.ds(off, BLK), :]
        out = []
        for h in range(2):
            m_row, l_row, acc = state[3 * h:3 * h + 3]
            s = nt(k_blk, q_half[h])
            if diag:
                kk = lax.broadcasted_iota(jnp.int32, (BLK, BLK), 0)
                qq = lax.broadcasted_iota(jnp.int32, (BLK, BLK), 1)
                s = jnp.where(kk <= qq, s, NEG_BIG)
            m_new = jnp.maximum(m_row, jnp.max(s, axis=0, keepdims=True))
            fac = jnp.exp2((m_row - m_new) * LOG2E)
            p = jnp.exp2((s - m_new) * LOG2E)
            l_row = l_row * fac + jnp.sum(p, axis=0, keepdims=True)
            vt = vt_ref[64 * h:64 * h + 64, pl.ds(off, BLK)]
            acc = acc * fac + nn(vt, p.astype(BF16))
            out += [m_new, l_row, acc]
        return tuple(out)

    fresh = (jnp.full((1, BLK), NEG_BIG, F32), jnp.zeros((1, BLK), F32), jnp.zeros((64, BLK), F32))
    state = lax.fori_loop(0, seq, lambda j, st: update(j, st, False), fresh + fresh)
    state = update(seq, state, True)
    o_t = jnp.concatenate([state[2] / state[1], state[5] / state[4]], axis=0)
    o_ref[pl.ds(q_off, BLK), :] = o_t.T.astype(BF16)
    for h in range(2):
        lse_ref[0, h:h + 1, pl.ds(q_off, BLK)] = (state[3 * h] + jnp.log(state[3 * h + 1])) * LOG2E

    @pl.when(step == 3)
    def _():
        for j in range(4):
            o_refs[j][...] = o_ref[pl.ds(j * BLK, BLK), :]


def attn_bwd_kernel(pair, tab_ref, *refs):
    qkv_refs, do_refs, o_refs, lse_refs, out_refs = refs[:8], refs[8:12], refs[12:20], refs[20:22], refs[22:26]
    q_ref, k_ref, v_ref, do_ref, o_ref, lse_ref, dqt_ref, dot_ref, dkv_ref, sem = refs[26:]
    n_blk = 8
    step = pl.program_id(0)

    @pl.when(step == 0)
    def _():
        load_all([[(r, 0, 384 * pair + 128 * t) for r in qkv_refs] for t in range(3)]
                 + [[(do_refs[b % 4], (b // 4) * BLK, 0) for b in range(8)], [(r, 0, 0) for r in o_refs]],
                 [q_ref, k_ref, v_ref, do_ref, o_ref], sem)
        dqt_ref[...] = jnp.zeros_like(dqt_ref)
        for i in range(2):
            lse_ref[:, i * 4 * BLK:(i + 1) * 4 * BLK] = lse_refs[i][0]
        for b in range(n_blk):
            rows = pl.ds(b * BLK, BLK)
            prod = (do_ref[rows, :].astype(F32) * o_ref[rows, :].astype(F32)).T
            dot_ref[0:1, rows] = jnp.sum(prod[:64], axis=0, keepdims=True)
            dot_ref[1:2, rows] = jnp.sum(prod[64:], axis=0, keepdims=True)

    k_off = pl.multiple_of(tab_ref[step] * BLK, BLK)
    k_blk = k_ref[pl.ds(k_off, BLK), :]
    v_blk = v_ref[pl.ds(k_off, BLK), :]
    k_t = k_blk.astype(F32).T.astype(BF16)

    def update(q_idx, state, diag):
        dk, dv = state
        off = pl.multiple_of(tab_ref[q_idx] * BLK, BLK)
        q_blk = q_ref[pl.ds(off, BLK), :] * jnp.asarray(0.125, BF16)
        do_blk = do_ref[pl.ds(off, BLK), :]
        for h in range(2):
            q_h = pick(q_blk, h)
            do_h = pick(do_blk, h)
            s = nt(k_blk, q_h)
            if diag:
                kk = lax.broadcasted_iota(jnp.int32, (BLK, BLK), 0)
                qq = lax.broadcasted_iota(jnp.int32, (BLK, BLK), 1)
                s = jnp.where(kk <= qq, s, NEG_BIG)
            p = jnp.exp2(s * LOG2E - lse_ref[h:h + 1, pl.ds(off, BLK)])
            dp = nt(v_blk, do_h).astype(BF16).astype(F32)
            ds = (p * (dp - dot_ref[h:h + 1, pl.ds(off, BLK)])).astype(BF16)
            dv = dv + nn(p.astype(BF16), do_h)
            dk = dk + nn(ds, q_h)
            cols = pl.ds(off, BLK)
            dqt_ref[64 * h:64 * h + 64, cols] += nn(k_t[64 * h:64 * h + 64], ds)
        return dk, dv

    zero = jnp.zeros((BLK, 128), F32)
    state = update(step, (zero, zero), True)
    dk, dv = lax.fori_loop(step + 1, n_blk, lambda i, st: update(i, st, False), state)
    dkv_ref[pl.ds(k_off, BLK), 0:128] = dk.astype(BF16)
    dkv_ref[pl.ds(k_off, BLK), 128:256] = dv.astype(BF16)

    @pl.when(step == n_blk - 1)
    def _():
        for b in range(n_blk):
            span = pl.ds(b * BLK, BLK)
            dst = pl.ds((b // 4) * BLK, BLK)
            out_refs[b % 4][dst, 0:128] = (dqt_ref[:, span] * 0.125).T.astype(BF16)
            out_refs[b % 4][dst, 128:384] = dkv_ref[span, :]


def pair_cost(n_pairs, n_dots):
    return pl.CostEstimate(flops=2 * n_pairs * BLK * BLK * 128 * n_dots * 6, bytes_accessed=2 ** 22,
                           transcendentals=2 * n_pairs * BLK * BLK)


ANY = pl.BlockSpec(memory_space=pl.ANY)


def attn_fwd(tab, qkv, pair, first):
    n_in = len(qkv)
    half = 4 * BLK
    buf = lambda n: pltpu.VMEM((n * BLK, 128), BF16)
    return pl.pallas_call(
        functools.partial(attn_fwd_kernel, pair, n_in, first),
        out_shape=[jax.ShapeDtypeStruct((BLK, 128), BF16)] * 4 + [jax.ShapeDtypeStruct((1, 2, half), F32)],
        grid_spec=pltpu.PrefetchScalarGridSpec(
            num_scalar_prefetch=1, grid=(4,),
            in_specs=[ANY] * n_in,
            out_specs=[pl.BlockSpec((BLK, 128), lambda i, tab: (0, 0))] * 4
                      + [pl.BlockSpec((1, 2, half), lambda i, tab: (0, 0, 0))],
            scratch_shapes=[buf(4), buf(n_in), buf(n_in), pltpu.VMEM((128, n_in * BLK), BF16), buf(4),
                            pltpu.SemaphoreType.DMA]),
        compiler_params=pltpu.CompilerParams(vmem_limit_bytes=48 * 1024 * 1024),
        cost_estimate=pair_cost(26 if first else 10, 2),
        name='attn_fwd')(tab, *qkv)


def attn_bwd(tab, qkv, d_o, out_o, lses, pair):
    seq_len = 8 * BLK
    buf = pltpu.VMEM((seq_len, 128), BF16)
    return pl.pallas_call(
        functools.partial(attn_bwd_kernel, pair),
        out_shape=[jax.ShapeDtypeStruct((2 * BLK, 384), BF16)] * 4,
        grid_spec=pltpu.PrefetchScalarGridSpec(
            num_scalar_prefetch=1, grid=(8,),
            in_specs=[ANY] * 20 + [pl.BlockSpec((1, 2, seq_len // 2), lambda i, tab: (0, 0, 0))] * 2,
            out_specs=[pl.BlockSpec((2 * BLK, 384), lambda i, tab: (0, 0))] * 4,
            scratch_shapes=[buf, buf, buf, buf, buf, pltpu.VMEM((2, seq_len), F32), pltpu.VMEM((128, seq_len), F32),
                            pltpu.VMEM((2, seq_len), F32), pltpu.VMEM((seq_len, 256), BF16), pltpu.SemaphoreType.DMA]),
        compiler_params=pltpu.CompilerParams(vmem_limit_bytes=48 * 1024 * 1024),
        cost_estimate=pair_cost(36, 5),
        name='attn_bwd')(tab, *qkv, *d_o, *out_o, *lses)


def attend_out_kernel(rank_ref, x_ref, wo_ref, *refs):
    parts, hid_ref, o_ref = refs[:16], refs[16], refs[17]
    for i in range(2):
        for j in range(4):
            for p in range(2):
                col = pl.multiple_of(rank_ref[1 + j] * 256 + 128 * p, 128)
                o_ref[pl.ds(i * BLK, BLK), pl.ds(col, 128)] = parts[8 * i + 2 * j + p][...]

    def tile(t, carry):
        rows = pl.ds(pl.multiple_of(t * 256, 256), 256)
        hid_ref[rows, :] = (x_ref[rows, :].astype(F32) + nn(o_ref[rows, :], wo_ref[...])).astype(BF16)
        return carry

    lax.fori_loop(0, x_ref.shape[0] // 256, tile, 0)


def attend_out(where, x, wo, parts):
    return pl.pallas_call(
        attend_out_kernel,
        out_shape=[jax.ShapeDtypeStruct(x.shape, BF16)] * 2,
        in_specs=[pl.BlockSpec(memory_space=pltpu.SMEM)] + [pl.BlockSpec(memory_space=pltpu.VMEM)] * 18,
        out_specs=[pl.BlockSpec(memory_space=pltpu.VMEM)] * 2,
        compiler_params=pltpu.CompilerParams(vmem_limit_bytes=32 * 1024 * 1024),
        cost_estimate=pl.CostEstimate(flops=2 ** 31, bytes_accessed=2 ** 23, transcendentals=0),
        name='attend_out')(where, x, wo, *parts)


def input_grad_kernel(where_ref, base_ref, w_ref, *refs):
    parts, out_ref = refs[:8], refs[8]
    acc = base_ref[...].astype(F32)
    for j in range(4):
        for p in range(2):
            row = pl.multiple_of((where_ref[1 + j] * 2 + p) * 384, 128)
            acc = acc + nn(parts[2 * j + p][...], w_ref[pl.ds(row, 384), :])
    out_ref[...] = acc.astype(BF16)


def input_grad(where, base, w_qkv, parts):
    rows, cols = base.shape
    tile = 256
    return pl.pallas_call(
        input_grad_kernel,
        out_shape=jax.ShapeDtypeStruct(base.shape, BF16),
        grid_spec=pltpu.PrefetchScalarGridSpec(
            num_scalar_prefetch=1, grid=(rows // tile,),
            in_specs=[pl.BlockSpec((tile, cols), lambda i, s: (i, 0)), pl.BlockSpec(w_qkv.shape, lambda i, s: (0, 0))]
                     + [pl.BlockSpec((tile, 384), lambda i, s: (i, 0))] * 8,
            out_specs=pl.BlockSpec((tile, cols), lambda i, s: (i, 0))),
        compiler_params=pltpu.CompilerParams(vmem_limit_bytes=40 * 1024 * 1024),
        cost_estimate=pl.CostEstimate(flops=6 * 2 ** 30, bytes_accessed=2 ** 24, transcendentals=0),
        name='input_grad')(where, base, w_qkv, *parts)


MESH = pl.DeviceIdType.MESH
LAG = 2
UNIT = 256
WIDE = 1024


def sum_kernel(up_ref, mine_ref, up_out, qkv_out, acc, rc, r1, r2, rz, macc, my, mz,
               one, pairs, tri_s, tri_r, tri_as, tri_ar, m_one, m_pairs, m_tri_s, m_tri_r, m_tri_as, m_tri_ar):
    dp, cp = lax.axis_index('dp'), lax.axis_index('cp')
    z, y, x, c = dp // 2, dp % 2, cp // 2, cp % 2
    n_up, n_mine = acc.shape[0], macc.shape[0]
    blocks = up_ref.shape[1] // WIDE
    ids = lambda d, p: {'dp': d, 'cp': p}
    core_id = ids(dp, 2 * x + 1 - c)
    x_id = ids(dp, 2 * (1 - x) + c)
    y_id = ids(2 * z + 1 - y, cp)
    z_ids = [ids(2 * ((z + k) % 4) + y, cp) for k in (1, 2, 3)]

    barrier = pltpu.get_barrier_semaphore()
    for peer in [core_id, x_id, y_id] + z_ids:
        pl.semaphore_signal(barrier, inc=1, device_id=peer, device_id_type=MESH)
    pl.semaphore_wait(barrier, 6)

    def remote(src, dst, s_sem, r_sem, dev):
        return pltpu.make_async_remote_copy(src_ref=src, dst_ref=dst, send_sem=s_sem, recv_sem=r_sem,
                                            device_id=dev, device_id_type=MESH)

    class Up:
        def __init__(self, u):
            color = u % 2
            self.u = u
            self.row = (u // blocks) * UNIT
            self.cols = pl.ds(pl.multiple_of((u % blocks) * WIDE, WIDE), WIDE)
            self.b1 = x + color * (y - x)
            self.b2 = y + color * (x - y)
            self.d1 = ids(2 * z + y + color * (1 - 2 * y), 2 * (x + (1 - color) * (1 - 2 * x)) + c)
            self.d2 = ids(2 * z + y + (1 - color) * (1 - 2 * y), 2 * (x + color * (1 - 2 * x)) + c)
            self.base = self.b1 * (UNIT // 4) + self.b2 * (UNIT // 8)

        def src(self, off, n):
            return up_ref.at[pl.ds(pl.multiple_of(self.row + off, 8), n), self.cols]

        def out(self, off, n):
            return up_out.at[pl.ds(pl.multiple_of(self.row + off, 8), n), self.cols]

        def part(self, off, n):
            return acc.at[self.u, pl.ds(pl.multiple_of(off, 8), n), :]

        def pair(self, i, src, dst, dev):
            return remote(src, dst, pairs.at[self.u, i, 0], pairs.at[self.u, i, 1], dev)

        def load(self):
            return pltpu.make_async_copy(self.src(c * (UNIT // 2), UNIT // 2), acc.at[self.u], one.at[self.u, 0])

        def core(self):
            return self.pair(0, self.src((1 - c) * (UNIT // 2), UNIT // 2), rc.at[self.u], core_id)

        def first(self):
            return self.pair(1, self.part((1 - self.b1) * (UNIT // 4), UNIT // 4), r1.at[self.u], self.d1)

        def second(self):
            return self.pair(2, self.part(self.b1 * (UNIT // 4) + (1 - self.b2) * (UNIT // 8), UNIT // 8),
                             r2.at[self.u], self.d2)

        def zs(self):
            n = UNIT // 32
            return [remote(self.part(self.base + ((z + k) % 4) * n, n), rz.at[self.u, k - 1],
                           tri_s.at[self.u, k - 1], tri_r.at[self.u, k - 1], z_ids[k - 1]) for k in (1, 2, 3)]

        def back_zs(self):
            n = UNIT // 32
            dst = self.out(c * (UNIT // 2) + self.base + z * n, n)
            return [remote(self.part(self.base + z * n, n), dst,
                           tri_as.at[self.u, k - 1], tri_ar.at[self.u, k - 1], z_ids[k - 1]) for k in (1, 2, 3)]

        def keep(self):
            n = UNIT // 32
            return pltpu.make_async_copy(self.part(self.base + z * n, n),
                                         self.out(c * (UNIT // 2) + self.base + z * n, n), one.at[self.u, 1])

        def back(self, i, off, n, dev):
            return self.pair(i, self.out(off, n), self.out(off, n), dev)

        def back_second(self):
            return self.back(3, c * (UNIT // 2) + self.base, UNIT // 8, self.d2)

        def back_first(self):
            return self.back(4, c * (UNIT // 2) + self.b1 * (UNIT // 4), UNIT // 4, self.d1)

        def back_core(self):
            return self.back(5, c * (UNIT // 2), UNIT // 2, core_id)

    def add_into(ref, other):
        ref[...] = ref[...] + other[...]

    def up_take(s, u):
        w = Up(u)
        if s == 1:
            w.load().wait()
            w.core().wait_recv()
            add_into(acc.at[u], rc.at[u])
        elif s == 2:
            w.first().wait_recv()
            add_into(w.part(w.b1 * (UNIT // 4), UNIT // 4), r1.at[u])
        elif s == 3:
            w.second().wait_recv()
            add_into(w.part(w.base, UNIT // 8), r2.at[u])
        elif s == 4:
            for cpy in w.zs():
                cpy.wait_recv()
            n = UNIT // 32
            dst = w.part(w.base + z * n, n)
            dst[...] = dst[...] + (rz[u, 0] + rz[u, 1] + rz[u, 2])
        elif s == 5:
            for cpy in w.back_zs():
                cpy.wait_recv()
            w.keep().wait()
        elif s == 6:
            w.back_second().wait_recv()
        elif s == 7:
            w.back_first().wait_recv()
        elif s == 8:
            w.back_core().wait_recv()
            for cpy in [w.core(), w.first(), w.second()] + w.zs() + w.back_zs() + [
                    w.back_second(), w.back_first(), w.back_core()]:
                cpy.wait_send()

    def up_give(s, u):
        w = Up(u)
        todo = [lambda: [w.load(), w.core()], lambda: [w.first()], lambda: [w.second()], w.zs,
                lambda: w.back_zs() + [w.keep()], lambda: [w.back_second()], lambda: [w.back_first()],
                lambda: [w.back_core()]][s]
        for cpy in todo():
            cpy.start()

    class Mine:
        def __init__(self, m):
            self.m = m
            self.orow = (m // 4) * 1024 + (m % 4) * 64

        def out(self, holder, off, n):
            return qkv_out.at[pl.ds(pl.multiple_of(self.orow + holder * 256 + off, 8), n), :]

        def part(self, off, n):
            return macc.at[self.m, pl.ds(pl.multiple_of(off, 8), n), :]

        def pair(self, i, src, dst, dev):
            return remote(src, dst, m_pairs.at[self.m, i, 0], m_pairs.at[self.m, i, 1], dev)

        def load(self):
            return pltpu.make_async_copy(mine_ref.at[pl.ds(pl.multiple_of(self.m * 64, 8), 64), :], macc.at[self.m],
                                         m_one.at[self.m, 0])

        def ys(self):
            return self.pair(0, mine_ref.at[pl.ds(pl.multiple_of(self.m * 64 + (1 - y) * 32, 8), 32), :],
                             my.at[self.m], y_id)

        def zs(self):
            return [remote(self.part(y * 32 + ((z + k) % 4) * 8, 8), mz.at[self.m, k - 1],
                           m_tri_s.at[self.m, k - 1], m_tri_r.at[self.m, k - 1], z_ids[k - 1]) for k in (1, 2, 3)]

        def back_zs(self):
            return [remote(self.part(y * 32 + z * 8, 8), self.out(cp, y * 32 + z * 8, 8),
                           m_tri_as.at[self.m, k - 1], m_tri_ar.at[self.m, k - 1], z_ids[k - 1]) for k in (1, 2, 3)]

        def keep(self):
            return pltpu.make_async_copy(self.part(y * 32 + z * 8, 8), self.out(cp, y * 32 + z * 8, 8),
                                         m_one.at[self.m, 1])

        def back_y(self):
            return self.pair(1, self.out(cp, y * 32, 32), self.out(cp, y * 32, 32), y_id)

        def back_x(self):
            return self.pair(2, self.out(cp, 0, 64), self.out(cp, 0, 64), x_id)

        def back_core(self):
            return self.pair(3, self.out(cp, 0, 64), self.out(cp, 0, 64), core_id)

        def back_far(self):
            far = 2 * (1 - x) + c
            return self.pair(4, self.out(far, 0, 64), self.out(far, 0, 64), core_id)

    def mine_take(s, m):
        w = Mine(m)
        if s == 1:
            w.load().wait()
            w.ys().wait_recv()
            add_into(w.part(y * 32, 32), my.at[m])
        elif s == 2:
            for cpy in w.zs():
                cpy.wait_recv()
            dst = w.part(y * 32 + z * 8, 8)
            dst[...] = dst[...] + (mz[m, 0] + mz[m, 1] + mz[m, 2])
        elif s == 3:
            for cpy in w.back_zs():
                cpy.wait_recv()
            w.keep().wait()
        elif s == 4:
            w.back_y().wait_recv()
        elif s == 5:
            w.back_x().wait_recv()
        elif s == 6:
            w.back_core().wait_recv()
            w.back_far().wait_recv()
            for cpy in [w.ys()] + w.zs() + w.back_zs() + [w.back_y(), w.back_x(), w.back_core(), w.back_far()]:
                cpy.wait_send()

    def mine_give(s, m):
        w = Mine(m)
        todo = [lambda: [w.load(), w.ys()], w.zs, lambda: w.back_zs() + [w.keep()], lambda: [w.back_y()],
                lambda: [w.back_x(), w.back_core()], lambda: [w.back_far()]][s]
        for cpy in todo():
            cpy.start()

    def at_step(fn, t, s, n):
        u = t - LAG * s

        @pl.when((u >= 0) & (u < n))
        def _():
            fn(s, u)

    def step(t, carry):
        for s in range(8, 0, -1):
            at_step(up_take, t, s, n_up)
        for s in range(6, 0, -1):
            at_step(mine_take, t, s, n_mine)
        for s in range(7, -1, -1):
            at_step(up_give, t, s, n_up)
        for s in range(5, -1, -1):
            at_step(mine_give, t, s, n_mine)
        return carry

    lax.fori_loop(0, max(n_up + 8 * LAG, n_mine + 6 * LAG), step, 0)


def sum_grads(up, mine):
    n_up = up.shape[0] * up.shape[1] // (UNIT * WIDE)
    n_mine = mine.shape[0] // 64
    cols = mine.shape[1]
    dma = pltpu.SemaphoreType.DMA
    vm = lambda *shape: pltpu.VMEM(shape, F32)
    return pl.pallas_call(
        sum_kernel,
        out_shape=[jax.ShapeDtypeStruct(up.shape, F32), jax.ShapeDtypeStruct((4 * mine.shape[0], cols), F32)],
        in_specs=[ANY] * 2, out_specs=[ANY] * 2,
        scratch_shapes=[vm(n_up, UNIT // 2, WIDE), vm(n_up, UNIT // 2, WIDE), vm(n_up, UNIT // 4, WIDE),
                        vm(n_up, UNIT // 8, WIDE), vm(n_up, 3, UNIT // 32, WIDE),
                        vm(n_mine, 64, cols), vm(n_mine, 32, cols), vm(n_mine, 3, 8, cols),
                        dma((n_up, 2)), dma((n_up, 6, 2))] + [dma((n_up, 3))] * 4
                       + [dma((n_mine, 2)), dma((n_mine, 5, 2))] + [dma((n_mine, 3))] * 4,
        compiler_params=pltpu.CompilerParams(collective_id=0, has_side_effects=True,
                                             vmem_limit_bytes=56 * 1024 * 1024),
        cost_estimate=pl.CostEstimate(flops=200 * 10 ** 9, bytes_accessed=2 ** 26, transcendentals=0),
        name='sum_grads')(up, mine)


def tn(a, b):
    return lax.dot_general(a, b, (((0,), (0,)), ((), ())), preferred_element_type=F32)


def solution(mesh):
    cp_size = mesh.shape['cp']
    n_total = mesh.shape['dp'] * cp_size
    inv = 1.0 / n_total

    def flip(arr, bit):
        return lax.ppermute(arr, 'cp', [(i, i ^ bit) for i in range(cp_size)]) if bit else arr

    def layer(x_in, d_out, w_q, w_k, w_v, w_o, w_up, w_down):
        rank = lax.axis_index('cp')
        x_own, g_out = x_in[0], d_out[0]
        tokens, d_model = x_own.shape
        width = d_model // cp_size
        n_pairs = width // 128
        slots = range(cp_size)
        halves = range(2)
        w_t = [jnp.transpose(w, (1, 2, 0)).reshape(d_model // 128, 1, 128, d_model) for w in (w_q, w_k, w_v)]
        w_qkv = jnp.concatenate(w_t, axis=1).reshape(3 * d_model, d_model)
        wo2 = w_o.reshape(d_model, d_model)
        w_mine = lax.dynamic_slice(w_qkv, (rank * 3 * width, 0), (3 * width, d_model))

        x_part = [x_own[:BLK], x_own[BLK:]]
        far = [flip(x_part[i], 2) for i in halves]
        near = [flip(x_part[i], 1) for i in halves]
        grad_act = nt(g_out, w_down).astype(BF16)
        far[0], grad_act = lax.optimization_barrier((far[0], grad_act))
        x_all = [[x_part[i], near[i], far[i], flip(far[i], 1)] for i in halves]
        seq_blk = jnp.arange(2 * cp_size)
        tab = jnp.where(seq_blk < cp_size, jnp.bitwise_xor(seq_blk, rank),
                        cp_size + jnp.bitwise_xor(2 * cp_size - 1 - seq_blk, rank)).astype(jnp.int32)
        qkv = [[nt(x_j, w_mine).astype(BF16) for x_j in x_all[i]] for i in halves]

        where = jnp.stack([rank] + [rank ^ j for j in slots]).astype(jnp.int32)
        attn_o, lses, o_parts = {}, {}, {}
        for i in halves:
            for pair in range(n_pairs):
                *o_slots, lses[pair, i] = attn_fwd(tab, qkv[0] + (qkv[1] if i else []), pair, 4 * i)
                attn_o[pair, i] = o_slots
                for j in slots:
                    o_parts[i, j, pair] = flip(o_slots[j], j)
        hidden, o_own = attend_out(where, x_own, wo2,
                                   [o_parts[i, j, p] for i in halves for j in slots for p in range(n_pairs)])
        up_pre = nn(hidden, w_up).astype(BF16)
        act_val, gelu_pull = jax.vjp(functools.partial(jax.nn.gelu, approximate=True), up_pre.astype(F32))
        act_b = act_val.astype(BF16)
        grad_pre = gelu_pull(grad_act.astype(F32))[0].astype(BF16)
        grad_down = tn(act_b, g_out) * inv
        grad_down = lax.psum(grad_down, ('dp', 'cp'))
        grad_hidden = (g_out.astype(F32) + nt(grad_pre, w_up)).astype(BF16)
        grad_attn = nt(grad_hidden, wo2).astype(BF16)

        d_o = []
        for pair in range(n_pairs):
            if pair:
                grad_attn, d_o[0] = lax.optimization_barrier((grad_attn, d_o[0]))
            pieces = [lax.dynamic_slice(grad_attn, (0, (rank ^ j) * width + 128 * pair), (tokens, 128)) for j in slots]
            d_o.append([flip(pieces[j], j) for j in slots])
            if not pair:
                grad_uo = jnp.concatenate([tn(hidden, grad_pre) * inv, tn(o_own, grad_hidden) * inv], axis=1)
                d_o[0], grad_uo = lax.optimization_barrier((d_o[0], grad_uo))

        grads, back = [], {}
        x_full = [jnp.concatenate([x_all[0][j], x_all[1][j]], axis=0) if j else x_own for j in slots]
        for pair in range(n_pairs):
            parts = attn_bwd(tab, qkv[0] + qkv[1], d_o[pair], attn_o[pair, 0] + attn_o[pair, 1],
                             [lses[pair, i] for i in halves], pair)
            for j in slots:
                back[j, pair] = flip(parts[j], j)
            grads.append(sum(tn(parts[j], x_full[j]) for j in slots) * inv)
        mine = jnp.concatenate(grads, axis=0).reshape(n_pairs, 3, 128, d_model)
        mine = jnp.transpose(mine, (1, 0, 2, 3)).reshape(3 * width, d_model)
        g_uo, g_qkv = sum_grads(grad_uo, mine)
        d_ff = w_up.shape[1]
        outs = [jnp.transpose(g_qkv[t * d_model:(t + 1) * d_model].reshape(w.shape[1], w.shape[2], d_model), (2, 0, 1))
                for t, w in enumerate((w_q, w_k, w_v))]
        d_x = input_grad(where, grad_hidden, w_qkv, [back[j, p] for j in slots for p in range(n_pairs)])
        return (d_x[None], *outs, g_uo[:, d_ff:].reshape(w_o.shape), g_uo[:, :d_ff], grad_down)

    act_spec = P('dp', 'cp', None)
    return jax.shard_map(layer, mesh=mesh,
                         in_specs=(act_spec, act_spec, P(), P(), P(), P(), P(), P()),
                         out_specs=(act_spec, P(), P(), P(), P(), P(), P()),
                         check_vma=False)
```

```python
import functools
import jax
import jax.numpy as jnp
from jax import lax
from jax.experimental import pallas as pl
from jax.experimental.pallas import tpu as pltpu
from jax.sharding import PartitionSpec as P


LOG2E = 1.4426950408889634
NEG_BIG = -1e30
BLK = 512
MIB = 2 ** 20
PAIR = range(2)
SLOTS = range(4)
FOLD = dict(axis=0, keepdims=True)
F32 = jnp.float32
BF16 = jnp.bfloat16


def nt(a, b):
    return lax.dot_general(a, b, (((1,), (1,)), ((), ())), preferred_element_type=F32)


def nn(a, b):
    return lax.dot_general(a, b, (((1,), (0,)), ((), ())), preferred_element_type=F32)


def lane_mask(half):
    lanes = lax.broadcasted_iota(jnp.int32, (BLK, 128), 1)
    return (lanes < 64) if half == 0 else (lanes >= 64)


def pick(arr, half):
    return jnp.where(lane_mask(half), arr, jnp.zeros_like(arr))


def load_all(srcs, dsts, sem):
    copies = []
    for parts, dst in zip(srcs, dsts):
        for b, (ref, row, col) in enumerate(parts):
            copies.append(pltpu.make_async_copy(ref.at[pl.ds(row, BLK), pl.ds(col, 128)],
                                                dst.at[pl.ds(b * BLK, BLK), :], sem))
    for c in copies:
        c.start()
    for c in copies:
        c.wait()


def attn_fwd_kernel(pair, n_in, first, tab_ref, *refs):
    qkv_refs, o_refs = refs[:n_in], refs[n_in:n_in + 4]
    lse_ref, q_ref, k_ref, v_ref, vt_ref, o_ref, sem = refs[n_in + 4:]
    step = pl.program_id(0)
    seq = step + first

    @pl.when(step == 0)
    def _():
        load_all([[(r, 0, 384 * pair + 128 * t) for r in (qkv_refs if t else qkv_refs[n_in - 4:])] for t in range(3)],
                 [q_ref, k_ref, v_ref], sem)
        for b in range(n_in):
            rows = pl.ds(b * BLK, BLK)
            vt_ref[:, rows] = v_ref[rows, :].astype(F32).T.astype(BF16)

    q_off = pl.multiple_of((tab_ref[seq] - first) * BLK, BLK)
    q_blk = q_ref[pl.ds(q_off, BLK), :] * jnp.asarray(0.125, BF16)
    q_half = [pick(q_blk, 0), pick(q_blk, 1)]

    def update(key_idx, state, diag):
        off = pl.multiple_of(tab_ref[key_idx] * BLK, BLK)
        k_blk = k_ref[pl.ds(off, BLK), :]
        out = []
        scores = [nt(k_blk, q_half[h]) for h in PAIR]
        for h in PAIR:
            m_row, l_row, acc = state[3 * h:3 * h + 3]
            s = scores[h]
            if diag:
                s = jnp.where(kept, s, NEG_BIG)
            m_new = jnp.maximum(m_row, jnp.max(s, **FOLD))
            fac = jnp.exp2((m_row - m_new) * LOG2E)
            p = jnp.exp2((s - m_new) * LOG2E)
            l_row = l_row * fac + jnp.sum(p, **FOLD)
            vt = vt_ref[64 * h:64 * h + 64, pl.ds(off, BLK)]
            acc = acc * fac + nn(vt, p.astype(BF16))
            out += [m_new, l_row, acc]
        return tuple(out)

    kept = lax.broadcasted_iota(jnp.int32, (BLK, BLK), 0) <= lax.broadcasted_iota(jnp.int32, (BLK, BLK), 1)
    fresh = (jnp.full((1, BLK), NEG_BIG, F32), jnp.zeros((1, BLK), F32), jnp.zeros((64, BLK), F32))
    state = lax.fori_loop(0, seq, lambda j, st: update(j, st, False), fresh + fresh)
    state = update(seq, state, True)
    o_t = jnp.concatenate([state[2] / state[1], state[5] / state[4]], axis=0)
    o_ref[pl.ds(q_off, BLK), :] = o_t.T.astype(BF16)
    for h in PAIR:
        lse_ref[0, h:h + 1, pl.ds(q_off, BLK)] = (state[3 * h] + jnp.log(state[3 * h + 1])) * LOG2E

    @pl.when(step == 3)
    def _():
        for j in SLOTS:
            o_refs[j][...] = o_ref[pl.ds(j * BLK, BLK), :]


def attn_bwd_kernel(pair, tab_ref, *refs):
    qkv_refs, do_refs, o_refs, lse_refs, out_refs = refs[:8], refs[8:12], refs[12:20], refs[20:22], refs[22:26]
    q_ref, k_ref, v_ref, do_ref, o_ref, lse_ref, dqt_ref, dot_ref, dkv_ref, sem = refs[26:]
    n_blk = 8
    step = pl.program_id(0)

    @pl.when(step == 0)
    def _():
        load_all([[(r, 0, 384 * pair + 128 * t) for r in qkv_refs] for t in range(3)]
                 + [[(do_refs[b % 4], (b // 4) * BLK, 0) for b in range(8)], [(r, 0, 0) for r in o_refs]],
                 [q_ref, k_ref, v_ref, do_ref, o_ref], sem)
        dqt_ref[...] = jnp.zeros_like(dqt_ref)
        for i in PAIR:
            lse_ref[:, i * 4 * BLK:(i + 1) * 4 * BLK] = lse_refs[i][0]
        for b in range(n_blk):
            rows = pl.ds(b * BLK, BLK)
            prod = (do_ref[rows, :].astype(F32) * o_ref[rows, :].astype(F32)).T
            dot_ref[0:1, rows] = jnp.sum(prod[:64], **FOLD)
            dot_ref[1:2, rows] = jnp.sum(prod[64:], **FOLD)

    k_off = pl.multiple_of(tab_ref[step] * BLK, BLK)
    k_blk = k_ref[pl.ds(k_off, BLK), :]
    v_blk = v_ref[pl.ds(k_off, BLK), :]
    k_t = k_blk.astype(F32).T.astype(BF16)

    def update(q_idx, state, diag):
        dk, dv = state
        off = pl.multiple_of(tab_ref[q_idx] * BLK, BLK)
        q_blk = q_ref[pl.ds(off, BLK), :] * jnp.asarray(0.125, BF16)
        do_blk = do_ref[pl.ds(off, BLK), :]
        for h in PAIR:
            q_h = pick(q_blk, h)
            do_h = pick(do_blk, h)
            s = nt(k_blk, q_h)
            if diag:
                kk = lax.broadcasted_iota(jnp.int32, (BLK, BLK), 0)
                qq = lax.broadcasted_iota(jnp.int32, (BLK, BLK), 1)
                s = jnp.where(kk <= qq, s, NEG_BIG)
            p = jnp.exp2(s * LOG2E - lse_ref[h:h + 1, pl.ds(off, BLK)])
            dp = nt(v_blk, do_h).astype(BF16).astype(F32)
            ds = (p * (dp - dot_ref[h:h + 1, pl.ds(off, BLK)])).astype(BF16)
            dv = dv + nn(p.astype(BF16), do_h)
            dk = dk + nn(ds, q_h)
            cols = pl.ds(off, BLK)
            dqt_ref[64 * h:64 * h + 64, cols] += nn(k_t[64 * h:64 * h + 64], ds)
        return dk, dv

    zero = jnp.zeros((BLK, 128), F32)
    state = update(step, (zero, zero), True)
    dk, dv = lax.fori_loop(step + 1, n_blk, lambda i, st: update(i, st, False), state)
    dkv_ref[pl.ds(k_off, BLK), 0:128] = dk.astype(BF16)
    dkv_ref[pl.ds(k_off, BLK), 128:256] = dv.astype(BF16)

    @pl.when(step == n_blk - 1)
    def _():
        for b in range(n_blk):
            span = pl.ds(b * BLK, BLK)
            dst = pl.ds((b // 4) * BLK, BLK)
            out_refs[b % 4][dst, 0:128] = (dqt_ref[:, span] * 0.125).T.astype(BF16)
            out_refs[b % 4][dst, 128:384] = dkv_ref[span, :]


def first_block(i, tab):
    return 0, 0


def first_block3(i, tab):
    return 0, 0, 0


def pair_cost(n_pairs, n_dots):
    return pl.CostEstimate(flops=2 * n_pairs * BLK * BLK * 128 * n_dots * 6, bytes_accessed=2 ** 22,
                           transcendentals=2 * n_pairs * BLK * BLK)


ANY = pl.BlockSpec(memory_space=pl.ANY)


def attn_fwd(tab, qkv, pair, first):
    n_in = len(qkv)
    half = 4 * BLK
    buf = lambda n: pltpu.VMEM((n * BLK, 128), BF16)
    return pl.pallas_call(
        functools.partial(attn_fwd_kernel, pair, n_in, first),
        out_shape=[jax.ShapeDtypeStruct((BLK, 128), BF16)] * 4 + [jax.ShapeDtypeStruct((1, 2, half), F32)],
        grid_spec=pltpu.PrefetchScalarGridSpec(
            num_scalar_prefetch=1, grid=(4,),
            in_specs=[ANY] * n_in,
            out_specs=[pl.BlockSpec((BLK, 128), first_block)] * 4
                      + [pl.BlockSpec((1, 2, half), first_block3)],
            scratch_shapes=[buf(4), buf(n_in), buf(n_in), pltpu.VMEM((128, n_in * BLK), BF16), buf(4),
                            pltpu.SemaphoreType.DMA]),
        compiler_params=pltpu.CompilerParams(vmem_limit_bytes=48 * MIB),
        cost_estimate=pair_cost(26 if first else 10, 2),
        name='attn_fwd')(tab, *qkv)


def attn_bwd(tab, qkv, d_o, out_o, lses, pair):
    seq_len = 8 * BLK
    buf = pltpu.VMEM((seq_len, 128), BF16)
    return pl.pallas_call(
        functools.partial(attn_bwd_kernel, pair),
        out_shape=[jax.ShapeDtypeStruct((2 * BLK, 384), BF16)] * 4,
        grid_spec=pltpu.PrefetchScalarGridSpec(
            num_scalar_prefetch=1, grid=(8,),
            in_specs=[ANY] * 20 + [pl.BlockSpec((1, 2, seq_len // 2), first_block3)] * 2,
            out_specs=[pl.BlockSpec((2 * BLK, 384), first_block)] * 4,
            scratch_shapes=[buf, buf, buf, buf, buf, pltpu.VMEM((2, seq_len), F32), pltpu.VMEM((128, seq_len), F32),
                            pltpu.VMEM((2, seq_len), F32), pltpu.VMEM((seq_len, 256), BF16), pltpu.SemaphoreType.DMA]),
        compiler_params=pltpu.CompilerParams(vmem_limit_bytes=48 * MIB),
        cost_estimate=pair_cost(36, 5),
        name='attn_bwd')(tab, *qkv, *d_o, *out_o, *lses)


def attend_out_kernel(rank_ref, x_ref, wo_ref, *refs):
    parts, hid_ref, o_ref = refs[:16], refs[16], refs[17]
    for i in PAIR:
        for j in SLOTS:
            for p in PAIR:
                col = pl.multiple_of(rank_ref[1 + j] * 256 + 128 * p, 128)
                o_ref[pl.ds(i * BLK, BLK), pl.ds(col, 128)] = parts[8 * i + 2 * j + p][...]

    def tile(t, carry):
        rows = pl.ds(pl.multiple_of(t * 256, 256), 256)
        hid_ref[rows, :] = (x_ref[rows, :].astype(F32) + nn(o_ref[rows, :], wo_ref[...])).astype(BF16)
        return carry

    lax.fori_loop(0, x_ref.shape[0] // 256, tile, 0)


def attend_out(where, x, wo, parts):
    return pl.pallas_call(
        attend_out_kernel,
        out_shape=[jax.ShapeDtypeStruct(x.shape, BF16)] * 2,
        in_specs=[pl.BlockSpec(memory_space=pltpu.SMEM)] + [pl.BlockSpec(memory_space=pltpu.VMEM)] * 18,
        out_specs=[pl.BlockSpec(memory_space=pltpu.VMEM)] * 2,
        compiler_params=pltpu.CompilerParams(vmem_limit_bytes=32 * MIB),
        cost_estimate=pl.CostEstimate(flops=2 ** 31, bytes_accessed=2 ** 23, transcendentals=0),
        name='attend_out')(where, x, wo, *parts)


def input_grad_kernel(where_ref, base_ref, w_ref, *refs):
    parts, out_ref = refs[:8], refs[8]
    acc = base_ref[...].astype(F32)
    for j in SLOTS:
        row = pl.multiple_of(where_ref[1 + j] * 768, 128)
        both = jnp.concatenate([parts[2 * j][...], parts[2 * j + 1][...]], axis=1)
        acc = acc + nn(both, w_ref[pl.ds(row, 768), :])
    out_ref[...] = acc.astype(BF16)


def input_grad(where, base, w_qkv, parts):
    rows, cols = base.shape
    tile = 256
    return pl.pallas_call(
        input_grad_kernel,
        out_shape=jax.ShapeDtypeStruct(base.shape, BF16),
        grid_spec=pltpu.PrefetchScalarGridSpec(
            num_scalar_prefetch=1, grid=(rows // tile,),
            in_specs=[pl.BlockSpec((tile, cols), lambda i, s: (i, 0)), pl.BlockSpec(w_qkv.shape, first_block)]
                     + [pl.BlockSpec((tile, 384), lambda i, s: (i, 0))] * 8,
            out_specs=pl.BlockSpec((tile, cols), lambda i, s: (i, 0))),
        compiler_params=pltpu.CompilerParams(vmem_limit_bytes=40 * MIB),
        cost_estimate=pl.CostEstimate(flops=6 * 2 ** 30, bytes_accessed=2 ** 24, transcendentals=0),
        name='input_grad')(where, base, w_qkv, *parts)


def qkv_grad_kernel(scale, *refs):
    parts, xs, out_ref, lt_ref = refs[:8], refs[8:16], refs[16], refs[17]
    for p in PAIR:
        for j in SLOTS:
            for i in PAIR:
                block = parts[4 * p + j][i * BLK:(i + 1) * BLK, :]
                lt_ref[:, pl.ds((4 * i + j) * BLK, BLK)] = block.astype(F32).T.astype(BF16)

        def tile(n, carry):
            cols = pl.ds(pl.multiple_of(n * 256, 256), 256)
            acc = nn(lt_ref[:, 0:BLK], xs[0][:, cols])
            for b in range(1, 8):
                acc = acc + nn(lt_ref[:, b * BLK:(b + 1) * BLK], xs[b][:, cols])
            out_ref[p * 384:(p + 1) * 384, cols] = acc * scale
            return carry

        lax.fori_loop(0, out_ref.shape[1] // 256, tile, 0)


def qkv_grad(scale, parts, xs):
    d_model = xs[0].shape[1]
    vmem = pl.BlockSpec(memory_space=pltpu.VMEM)
    return pl.pallas_call(
        functools.partial(qkv_grad_kernel, scale),
        out_shape=jax.ShapeDtypeStruct((768, d_model), F32),
        in_specs=[vmem] * 16, out_specs=vmem,
        scratch_shapes=[pltpu.VMEM((384, 8 * BLK), BF16)],
        compiler_params=pltpu.CompilerParams(vmem_limit_bytes=48 * MIB),
        cost_estimate=pl.CostEstimate(flops=6 * 2 ** 30, bytes_accessed=2 ** 24, transcendentals=0),
        name='qkv_grad')(*parts, *xs)


MESH = pl.DeviceIdType.MESH
LAG = 2
UNIT = 256
WIDE = 1024
HALF, QUART, EIGHTH, LEAF = UNIT // 2, UNIT // 4, UNIT // 8, UNIT // 32
HOPS = (1, 2, 3)
MROW = 64
MHALF = 32
ROW = 8
BIG = 1024
HELD = 256


def sum_kernel(up_ref, mine_ref, up_out, qkv_out, acc, rc, r1, r2, rz, macc, my, mz,
               one, pairs, tri_s, tri_r, tri_as, tri_ar, m_one, m_pairs, m_tri_s, m_tri_r, m_tri_as, m_tri_ar):
    dp, cp = lax.axis_index('dp'), lax.axis_index('cp')
    z, y, x, c = dp // 2, dp % 2, cp // 2, cp % 2
    n_up, n_mine = acc.shape[0], macc.shape[0]
    blocks = up_ref.shape[1] // WIDE
    ids = lambda d, p: {'dp': d, 'cp': p}
    core_id = ids(dp, 2 * x + 1 - c)
    x_id = ids(dp, 2 * (1 - x) + c)
    y_id = ids(2 * z + 1 - y, cp)
    z_ids = [ids(2 * ((z + k) % 4) + y, cp) for k in HOPS]

    barrier = pltpu.get_barrier_semaphore()
    for peer in [core_id, x_id, y_id] + z_ids:
        pl.semaphore_signal(barrier, inc=1, device_id=peer, device_id_type=MESH)
    pl.semaphore_wait(barrier, 6)

    def remote(src, dst, s_sem, r_sem, dev):
        return pltpu.make_async_remote_copy(src_ref=src, dst_ref=dst, send_sem=s_sem, recv_sem=r_sem,
                                            device_id=dev, device_id_type=MESH)

    class Up:
        def __init__(self, u):
            color = (u % 3 + 2) // 3
            self.u = u
            self.row = (u // blocks) * UNIT
            self.cols = pl.ds(pl.multiple_of((u % blocks) * WIDE, WIDE), WIDE)
            self.b1 = x + color * (y - x)
            self.b2 = y + color * (x - y)
            self.d1 = ids(2 * z + y + color * (1 - 2 * y), 2 * (x + (1 - color) * (1 - 2 * x)) + c)
            self.d2 = ids(2 * z + y + (1 - color) * (1 - 2 * y), 2 * (x + color * (1 - 2 * x)) + c)
            self.base = self.b1 * QUART + self.b2 * EIGHTH

        def src(self, off, n):
            return up_ref.at[pl.ds(pl.multiple_of(self.row + off, ROW), n), self.cols]

        def out(self, off, n):
            return up_out.at[pl.ds(pl.multiple_of(self.row + off, ROW), n), self.cols]

        def part(self, off, n):
            return acc.at[self.u, pl.ds(pl.multiple_of(off, ROW), n), :]

        def pair(self, i, src, dst, dev):
            return remote(src, dst, pairs.at[self.u, i, 0], pairs.at[self.u, i, 1], dev)

        def load(self):
            return pltpu.make_async_copy(self.src(c * HALF, HALF), acc.at[self.u], one.at[self.u, 0])

        def core(self):
            return self.pair(0, self.src((1 - c) * HALF, HALF), rc.at[self.u], core_id)

        def first(self):
            return self.pair(1, self.part((1 - self.b1) * QUART, QUART), r1.at[self.u], self.d1)

        def second(self):
            return self.pair(2, self.part(self.b1 * QUART + (1 - self.b2) * EIGHTH, EIGHTH),
                             r2.at[self.u], self.d2)

        def zs(self):
            n = LEAF
            return [remote(self.part(self.base + ((z + k) % 4) * n, n), rz.at[self.u, k - 1],
                           tri_s.at[self.u, k - 1], tri_r.at[self.u, k - 1], z_ids[k - 1]) for k in HOPS]

        def back_zs(self):
            n = LEAF
            dst = self.out(c * HALF + self.base + z * n, n)
            return [remote(self.part(self.base + z * n, n), dst,
                           tri_as.at[self.u, k - 1], tri_ar.at[self.u, k - 1], z_ids[k - 1]) for k in HOPS]

        def keep(self):
            n = LEAF
            return pltpu.make_async_copy(self.part(self.base + z * n, n),
                                         self.out(c * HALF + self.base + z * n, n), one.at[self.u, 1])

        def back(self, i, off, n, dev):
            return self.pair(i, self.out(off, n), self.out(off, n), dev)

        def back_second(self):
            return self.back(3, c * HALF + self.base, EIGHTH, self.d2)

        def back_first(self):
            return self.back(4, c * HALF + self.b1 * QUART, QUART, self.d1)

        def back_core(self):
            return self.back(5, c * HALF, HALF, core_id)

    def add_into(ref, other):
        ref[...] = ref[...] + other[...]

    def up_take(s, u):
        w = Up(u)
        if s == 1:
            w.load().wait()
            w.core().wait_recv()
            add_into(acc.at[u], rc.at[u])
        elif s == 2:
            w.first().wait_recv()
            add_into(w.part(w.b1 * QUART, QUART), r1.at[u])
        elif s == 3:
            w.second().wait_recv()
            add_into(w.part(w.base, EIGHTH), r2.at[u])
        elif s == 4:
            for cpy in w.zs():
                cpy.wait_recv()
            n = LEAF
            dst = w.part(w.base + z * n, n)
            dst[...] = dst[...] + (rz[u, 0] + rz[u, 1] + rz[u, 2])
        elif s == 5:
            for cpy in w.back_zs():
                cpy.wait_recv()
            w.keep().wait()
        elif s == 6:
            w.back_second().wait_recv()
        elif s == 7:
            w.back_first().wait_recv()
        elif s == 8:
            w.back_core().wait_recv()
            for cpy in [w.core(), w.first(), w.second()] + w.zs() + w.back_zs() + [
                    w.back_second(), w.back_first(), w.back_core()]:
                cpy.wait_send()

    def up_give(s, u):
        w = Up(u)
        todo = [lambda: [w.load(), w.core()], lambda: [w.first()], lambda: [w.second()], w.zs,
                lambda: w.back_zs() + [w.keep()], lambda: [w.back_second()], lambda: [w.back_first()],
                lambda: [w.back_core()]][s]
        for cpy in todo():
            cpy.start()

    class Mine:
        def __init__(self, m):
            self.m = m
            self.orow = (m % 6) // 2 * BIG + m // 6 * 128 + m % 2 * MROW

        def out(self, holder, off, n):
            return qkv_out.at[pl.ds(pl.multiple_of(self.orow + holder * HELD + off, ROW), n), :]

        def part(self, off, n):
            return macc.at[self.m, pl.ds(pl.multiple_of(off, ROW), n), :]

        def pair(self, i, src, dst, dev):
            return remote(src, dst, m_pairs.at[self.m, i, 0], m_pairs.at[self.m, i, 1], dev)

        def load(self):
            return pltpu.make_async_copy(mine_ref.at[pl.ds(pl.multiple_of(self.m * MROW, ROW), MROW), :], macc.at[self.m],
                                         m_one.at[self.m, 0])

        def ys(self):
            return self.pair(0, mine_ref.at[pl.ds(pl.multiple_of(self.m * MROW + (1 - y) * MHALF, ROW), MHALF), :],
                             my.at[self.m], y_id)

        def zs(self):
            return [remote(self.part(y * MHALF + ((z + k) % 4) * ROW, ROW), mz.at[self.m, k - 1],
                           m_tri_s.at[self.m, k - 1], m_tri_r.at[self.m, k - 1], z_ids[k - 1]) for k in HOPS]

        def back_zs(self):
            return [remote(self.part(y * MHALF + z * ROW, ROW), self.out(cp, y * MHALF + z * ROW, ROW),
                           m_tri_as.at[self.m, k - 1], m_tri_ar.at[self.m, k - 1], z_ids[k - 1]) for k in HOPS]

        def keep(self):
            return pltpu.make_async_copy(self.part(y * MHALF + z * ROW, ROW), self.out(cp, y * MHALF + z * ROW, ROW),
                                         m_one.at[self.m, 1])

        def back_y(self):
            return self.pair(1, self.out(cp, y * MHALF, MHALF), self.out(cp, y * MHALF, MHALF), y_id)

        def back_x(self):
            return self.pair(2, self.out(cp, 0, MROW), self.out(cp, 0, MROW), x_id)

        def back_core(self):
            return self.pair(3, self.out(cp, 0, MROW), self.out(cp, 0, MROW), core_id)

        def back_far(self):
            far = 2 * (1 - x) + c
            return self.pair(4, self.out(far, 0, MROW), self.out(far, 0, MROW), core_id)

    def mine_take(s, m):
        w = Mine(m)
        if s == 1:
            w.load().wait()
            w.ys().wait_recv()
            add_into(w.part(y * MHALF, MHALF), my.at[m])
        elif s == 2:
            for cpy in w.zs():
                cpy.wait_recv()
            dst = w.part(y * MHALF + z * ROW, ROW)
            dst[...] = dst[...] + (mz[m, 0] + mz[m, 1] + mz[m, 2])
        elif s == 3:
            for cpy in w.back_zs():
                cpy.wait_recv()
            w.keep().wait()
        elif s == 4:
            w.back_y().wait_recv()
        elif s == 5:
            w.back_x().wait_recv()
        elif s == 6:
            w.back_core().wait_recv()
            w.back_far().wait_recv()
            for cpy in [w.ys()] + w.zs() + w.back_zs() + [w.back_y(), w.back_x(), w.back_core(), w.back_far()]:
                cpy.wait_send()

    def mine_give(s, m):
        w = Mine(m)
        todo = [lambda: [w.load(), w.ys()], w.zs, lambda: w.back_zs() + [w.keep()], lambda: [w.back_y()],
                lambda: [w.back_x(), w.back_core()], lambda: [w.back_far()]][s]
        for cpy in todo():
            cpy.start()

    def at_step(fn, t, s, n):
        u = t - LAG * s

        @pl.when((u >= 0) & (u < n))
        def _():
            fn(s, u)

    def step(t, carry):
        for s in range(8, 0, -1):
            at_step(up_take, t, s, n_up)
        for s in range(6, 0, -1):
            at_step(mine_take, t, s, n_mine)
        for s in range(7, -1, -1):
            at_step(up_give, t, s, n_up)
        for s in range(5, -1, -1):
            at_step(mine_give, t, s, n_mine)
        return carry

    lax.fori_loop(0, max(n_up + 8 * LAG, n_mine + 6 * LAG), step, 0)


def sum_grads(up, mine):
    n_up = up.shape[0] * up.shape[1] // (UNIT * WIDE)
    n_mine = mine.shape[0] // MROW
    cols = mine.shape[1]
    dma = pltpu.SemaphoreType.DMA
    vm = lambda *shape: pltpu.VMEM(shape, F32)
    return pl.pallas_call(
        sum_kernel,
        out_shape=[jax.ShapeDtypeStruct(up.shape, F32), jax.ShapeDtypeStruct((4 * mine.shape[0], cols), F32)],
        in_specs=[ANY] * 2, out_specs=[ANY] * 2,
        scratch_shapes=[vm(n_up, UNIT // 2, WIDE), vm(n_up, UNIT // 2, WIDE), vm(n_up, UNIT // 4, WIDE),
                        vm(n_up, UNIT // 8, WIDE), vm(n_up, 3, UNIT // 32, WIDE),
                        vm(n_mine, MROW, cols), vm(n_mine, MHALF, cols), vm(n_mine, 3, ROW, cols),
                        dma((n_up, 2)), dma((n_up, 6, 2))] + [dma((n_up, 3))] * 4
                       + [dma((n_mine, 2)), dma((n_mine, 5, 2))] + [dma((n_mine, 3))] * 4,
        compiler_params=pltpu.CompilerParams(collective_id=0, has_side_effects=True,
                                             vmem_limit_bytes=56 * MIB),
        cost_estimate=pl.CostEstimate(flops=200 * 10 ** 9, bytes_accessed=2 ** 26, transcendentals=0),
        name='sum_grads')(up, mine)


def tn(a, b):
    return lax.dot_general(a, b, (((0,), (0,)), ((), ())), preferred_element_type=F32)


def solution(mesh):
    cp_size = mesh.shape['cp']
    n_total = mesh.shape['dp'] * cp_size
    inv = 1.0 / n_total

    def flip(arr, bit):
        return lax.ppermute(arr, 'cp', [(i, i ^ bit) for i in range(cp_size)]) if bit else arr

    def layer(x_in, d_out, w_q, w_k, w_v, w_o, w_up, w_down):
        rank = lax.axis_index('cp')
        x_own, g_out = x_in[0], d_out[0]
        tokens, d_model = x_own.shape
        width = d_model // cp_size
        n_pairs = width // 128
        slots = range(cp_size)
        halves = PAIR
        w_t = [jnp.transpose(w, (1, 2, 0)).reshape(d_model // 128, 1, 128, d_model) for w in (w_q, w_k, w_v)]
        w_qkv = jnp.concatenate(w_t, axis=1).reshape(3 * d_model, d_model)
        wo2 = w_o.reshape(d_model, d_model)
        w_mine = lax.dynamic_slice(w_qkv, (rank * 3 * width, 0), (3 * width, d_model))

        x_part = [x_own[:BLK], x_own[BLK:]]
        far = [flip(x_part[i], 2) for i in halves]
        near = [flip(x_part[i], 1) for i in halves]
        grad_act = nt(g_out, w_down).astype(BF16)
        far[0], grad_act = lax.optimization_barrier((far[0], grad_act))
        x_all = [[x_part[i], near[i], far[i], flip(far[i], 1)] for i in halves]
        seq_blk = jnp.arange(2 * cp_size)
        tab = jnp.where(seq_blk < cp_size, jnp.bitwise_xor(seq_blk, rank),
                        cp_size + jnp.bitwise_xor(2 * cp_size - 1 - seq_blk, rank)).astype(jnp.int32)
        qkv = [[nt(x_j, w_mine).astype(BF16) for x_j in x_all[i]] for i in halves]

        where = jnp.stack([rank] + [rank ^ j for j in slots]).astype(jnp.int32)
        attn_o, lses, o_parts = {}, {}, {}
        for i in halves:
            for pair in range(n_pairs):
                *o_slots, lses[pair, i] = attn_fwd(tab, qkv[0] + (qkv[1] if i else []), pair, 4 * i)
                attn_o[pair, i] = o_slots
                for j in slots:
                    o_parts[i, j, pair] = flip(o_slots[j], j)
        hidden, o_own = attend_out(where, x_own, wo2,
                                   [o_parts[i, j, p] for i in halves for j in slots for p in range(n_pairs)])
        up_pre = nn(hidden, w_up).astype(BF16)
        act_val, gelu_pull = jax.vjp(functools.partial(jax.nn.gelu, approximate=True), up_pre.astype(F32))
        act_b = act_val.astype(BF16)
        grad_pre = gelu_pull(grad_act.astype(F32))[0].astype(BF16)
        grad_down = tn(act_b, g_out) * inv
        grad_hidden = (g_out.astype(F32) + nt(grad_pre, w_up)).astype(BF16)
        grad_attn = nt(grad_hidden, wo2).astype(BF16)

        d_o = []
        for pair in range(n_pairs):
            if pair:
                grad_attn, d_o[0] = lax.optimization_barrier((grad_attn, d_o[0]))
            pieces = [lax.dynamic_slice(grad_attn, (0, (rank ^ j) * width + 128 * pair), (tokens, 128)) for j in slots]
            d_o.append([flip(pieces[j], j) for j in slots])
            if not pair:
                grad_up = tn(hidden, grad_pre)
                grad_o = tn(o_own, grad_hidden) * inv
                d_o[0], grad_up = lax.optimization_barrier((d_o[0], grad_up))
                grad_down, grad_o = lax.psum((grad_down, grad_o), ('dp', 'cp'))

        grads, back = [], {}
        for pair in range(n_pairs):
            parts = attn_bwd(tab, qkv[0] + qkv[1], d_o[pair], attn_o[pair, 0] + attn_o[pair, 1],
                             [lses[pair, i] for i in halves], pair)
            for j in slots:
                back[j, pair] = flip(parts[j], j)
            grads += parts
        mine = qkv_grad(inv, grads, x_all[0] + x_all[1])
        g_up, g_qkv = sum_grads(grad_up, mine)
        g_up = g_up * inv
        outs = [jnp.transpose(g_qkv[t * d_model:(t + 1) * d_model].reshape(w.shape[1], w.shape[2], d_model), (2, 0, 1))
                for t, w in enumerate((w_q, w_k, w_v))]
        d_x = input_grad(where, grad_hidden, w_qkv, [back[j, p] for j in slots for p in range(n_pairs)])
        return (d_x[None], *outs, grad_o.reshape(w_o.shape), g_up, grad_down)

    act_spec = P('dp', 'cp', None)
    return jax.shard_map(layer, mesh=mesh,
                         in_specs=(act_spec, act_spec, P(), P(), P(), P(), P(), P()),
                         out_specs=(act_spec, P(), P(), P(), P(), P(), P()),
                         check_vma=False)
```
